32 devices in a mesh: dp: 8 (over y, x, core), tensor: 4 (over z).
Axes of the slice: x: 2, y: 2, z: 4, core: 2. Of those that a mesh axis runs over, the one named last changes fastest.
Arguments:
- img_hidden: bfloat16 [4096, 4304], P('dp', 'tensor'), may hold values from -0.25 to 0.25
- img_down: bfloat16 [4304, 1152], P('tensor'), may hold values from -0.09375 to 0.09375
- img_pooled: bfloat16 [4096, 1152], P(('dp', 'tensor')), may hold values from -0.25 to 0.25
- txt_hidden: bfloat16 [4096, 1152], P('dp', 'tensor'), may hold values from -0.25 to 0.25
- txt_proj: bfloat16 [1152, 1152], P('tensor'), may hold values from -0.1875 to 0.1875
- log_temp: float32 [1], replicated, may hold values from 1 to 2
- bias: float32 [1], replicated, may hold values from -4 to -1
- match: int32 [4096], P(('dp', 'tensor')), may hold values from 0 to 4095
- window_index: int32 [1], replicated, may hold values from 0 to 1
Outputs:
- img_grad: float32 [4096, 1152], P(('dp', 'tensor'))
- txt_grad: float32 [4096, 1152], P(('dp', 'tensor'))
- row_loss: float32 [4096], P(('dp', 'tensor'))
The draws below stay inside these ranges and needn't reach their ends.
All inputs are finite; a program needn't handle non-finite values.
Results may differ from the reference program's by a relative error of at most 0.0039.
Values may be sent and summed in bfloat16 or wider, within the bound.
A program may use at most 64 MiB of HBM per device.

```python
import jax
import jax.numpy as jnp
from jax import lax

D = 1152
K_IMG = 4304
K_TXT = 1152
ROWS = 128
STEPS = 16
BATCH = 4096
WINDOWS = 2
N_DP = 8
N_TENSOR = 4


def plant(values, key, low, top_value):
    spot = [jax.random.randint(jax.random.fold_in(key, axis), (), 0, length) for axis, length in enumerate(values.shape)]
    main_axis = values.shape.index(max(values.shape))
    neighbour = spot[:main_axis] + [(spot[main_axis] + 1) % values.shape[main_axis]] + spot[main_axis + 1:]
    return values.at[tuple(spot)].set(low).at[tuple(neighbour)].set(top_value)


def block_scale(stream_key, dims, shards, smallest, largest):
    level = 1.0
    for dim, parts in shards:
        steps = jax.random.uniform(jax.random.fold_in(jax.random.fold_in(stream_key, 6), dim), (parts,), jnp.float32, smallest / len(shards), largest / len(shards))
        level = level * jnp.repeat(jnp.exp(steps), dims[dim] // parts).reshape((-1,) + (1,) * (len(dims) - 1 - dim))
    return level


def noise(rng, shape, scale, bound, split=(), kind=jnp.bfloat16):
    gain = block_scale(rng, shape, split, -0.22, 0.18) if split else 1.0
    array = jax.random.normal(rng, shape, jnp.float32) * scale * gain
    return jnp.minimum(jnp.maximum(array, -bound), bound).astype(kind)


def setup_inputs(seed: int = 0) -> dict:
    streams_of = jax.random.split(jax.random.key(seed), 10)
    img_hidden = noise(streams_of[0], (BATCH, K_IMG), 0.03125, 0.25, ((0, 8), (1, 4)))
    img_down = noise(streams_of[1], (K_IMG, D), K_IMG ** -0.5, 0.09375, ((0, 4),))
    img_pooled = noise(streams_of[2], (BATCH, D), 0.03125, 0.25, ((0, 32),))
    txt_hidden = noise(streams_of[3], (BATCH, K_TXT), 0.03125, 0.25, ((0, 8), (1, 4)))
    txt_proj = noise(streams_of[4], (K_TXT, D), K_TXT ** -0.5, 0.1875, ((0, 4),))
    log_temp = jnp.clip(jax.random.uniform(streams_of[5], (1,), jnp.float32, 1.0, 2.0), 1.0, 2.0)
    bias = jnp.clip(jax.random.uniform(streams_of[6], (1,), jnp.float32, -4.0, -1.0), -4.0, -1.0)
    match = plant(jax.random.randint(streams_of[7], (BATCH,), 0, BATCH), jax.random.fold_in(streams_of[7], 1), 0, BATCH - 1).astype(jnp.int32)
    window_index = jax.random.randint(streams_of[8], (1,), 0, WINDOWS).astype(jnp.int32)
    return {"img_hidden": img_hidden, "img_down": img_down, "img_pooled": img_pooled, "txt_hidden": txt_hidden, "txt_proj": txt_proj, "log_temp": log_temp, "bias": bias, "match": match, "window_index": window_index}


def unit_rows(emb):
    length = jnp.sqrt(lax.optimization_barrier(jnp.sum(emb * emb, axis=1, keepdims=True)) + 1e-06)
    return (emb / length, length)

def reference(img_hidden, img_down, img_pooled, txt_hidden, txt_proj, log_temp, bias, match, window_index):
    img_emb = jnp.dot(img_hidden, img_down, preferred_element_type=jnp.float32) + img_pooled.astype(jnp.float32)
    txt_emb = jnp.dot(txt_hidden, txt_proj, preferred_element_type=jnp.float32)
    img_unit, img_len = unit_rows(img_emb)
    txt_unit, txt_len = unit_rows(txt_emb)
    blocks = N_DP * N_TENSOR
    image_low = img_unit.astype(jnp.bfloat16).astype(jnp.float32).reshape(blocks, ROWS, D)
    text_low = txt_unit.astype(jnp.bfloat16).astype(jnp.float32).reshape(blocks, ROWS, D)
    scale = jnp.exp(log_temp[0])
    shift_value = bias[0]
    base = window_index[0] * STEPS
    match_blocks = match.reshape(blocks, ROWS)
    owners_base = jnp.arange(blocks, dtype=jnp.int32)
    row_offsets = jnp.arange(ROWS, dtype=jnp.int32)
    image_dunit = jnp.zeros((blocks, ROWS, D), jnp.float32)
    text_dunit = jnp.zeros((blocks, ROWS, D), jnp.float32)
    row_loss = jnp.zeros((blocks, ROWS), jnp.float32)
    for offset_step in range(STEPS):
        offset = (base + offset_step).astype(jnp.int32)
        texts = jnp.roll(text_low, offset, axis=0)
        owners = (owners_base - offset) % blocks
        text_index = owners[:, None] * ROWS + row_offsets[None, :]
        positive = match_blocks[:, :, None] == text_index[:, None, :]
        cosine = jnp.einsum('prd,pqd->prq', image_low, texts)
        logit = scale * cosine + shift_value
        row_loss = row_loss + lax.optimization_barrier(jnp.sum(jnp.where(positive, jax.nn.softplus(-logit), jax.nn.softplus(logit)), axis=2))
        coef = ((jax.nn.sigmoid(logit) - positive.astype(jnp.float32)) * scale).astype(jnp.bfloat16).astype(jnp.float32)
        image_dunit = image_dunit + jnp.einsum('prq,pqd->prd', coef, texts)
        text_dunit = text_dunit + jnp.roll(jnp.einsum('prq,prd->pqd', coef, image_low), -offset, axis=0)
    image_dunit = image_dunit.reshape(BATCH, D)
    text_dunit = text_dunit.reshape(BATCH, D)
    img_grad = (image_dunit - img_unit * lax.optimization_barrier(jnp.sum(img_unit * image_dunit, axis=1, keepdims=True))) / img_len
    txt_grad = (text_dunit - txt_unit * lax.optimization_barrier(jnp.sum(txt_unit * text_dunit, axis=1, keepdims=True))) / txt_len
    return (img_grad, txt_grad, row_loss.reshape(BATCH))
```

```python
import jax
import jax.numpy as jnp
from jax import lax
from jax.experimental import pallas as pl
from jax.experimental.pallas import tpu as pltpu
from jax.sharding import PartitionSpec as P

STEPS = 16


def shifted(shard, axis, by):
    devices = lax.axis_size(axis)
    return lax.ppermute(shard, axis, [(i, (i + by) % devices) for i in range(devices)])


def unit_rows(emb):
    length = jnp.sqrt(jnp.sum(emb * emb, axis=1, keepdims=True) + 1e-06)
    return (emb / length, length)


def pair_tile(image_low, text_block, owner, match, scale, shift_value):
    cosine = lax.dot_general(
        image_low, text_block, (((1,), (1,)), ((), ())), preferred_element_type=jnp.float32
    )
    text_index = owner * text_block.shape[0] + lax.iota(jnp.int32, text_block.shape[0])
    positive = match[:, None] == text_index[None, :]
    logit = scale * cosine + shift_value
    pair_loss = jnp.sum(
        jnp.where(positive, jax.nn.softplus(-logit), jax.nn.softplus(logit)), axis=1
    )
    coef = ((jax.nn.sigmoid(logit) - positive.astype(jnp.float32)) * scale).astype(jnp.bfloat16)
    image_part = jnp.dot(coef, text_block, preferred_element_type=jnp.float32)
    text_part = lax.dot_general(
        coef, image_low, (((0,), (0,)), ((), ())), preferred_element_type=jnp.float32
    )
    return (pair_loss, image_part, text_part)


def offset_blocks(blocks, window):
    windows = lax.axis_size(("dp", "tensor")) // STEPS
    for level in range((windows - 1).bit_length()):
        moved = shifted(blocks, ("dp", "tensor"), STEPS << level)
        blocks = jnp.where(window >> level & 1 == 1, moved, blocks)
    return blocks


def return_home(text_sum, fixed_steps, window):
    text_sum = shifted(text_sum, ("dp", "tensor"), -fixed_steps)
    windows = lax.axis_size(("dp", "tensor")) // STEPS
    for level in range((windows - 1).bit_length()):
        moved = shifted(text_sum, ("dp", "tensor"), -(STEPS << level))
        text_sum = jnp.where(window >> level & 1 == 1, moved, text_sum)
    return text_sum


def ring_body(
    img_hidden, img_down, img_pooled, txt_hidden, txt_proj, log_temp, bias, match, window_index
):
    width = img_pooled.shape[1]
    summed = lax.psum_scatter(
        jnp.concatenate(
            [
                jnp.dot(img_hidden, img_down, preferred_element_type=jnp.float32),
                jnp.dot(txt_hidden, txt_proj, preferred_element_type=jnp.float32),
            ],
            axis=1,
        ),
        "tensor",
        scatter_dimension=0,
        tiled=True,
    )
    img_emb = summed[:, :width] + img_pooled.astype(jnp.float32)
    txt_emb = summed[:, width:]
    img_unit, img_len = unit_rows(img_emb)
    txt_unit, txt_len = unit_rows(txt_emb)
    image_low = img_unit.astype(jnp.bfloat16)
    text_low = txt_unit.astype(jnp.bfloat16)
    scale = jnp.exp(log_temp[0])
    shift_value = bias[0]
    window = window_index[0]
    start_step = window * STEPS
    position = lax.axis_index(("dp", "tensor"))
    devices = lax.axis_size(("dp", "tensor"))
    half_steps = STEPS // 2
    late_copy = shifted(text_low, ("dp", "tensor"), STEPS - 1)
    stacked = offset_blocks(jnp.stack([text_low, late_copy]), window)
    early_block = stacked[0]
    late_block = stacked[1]
    early_owner = (position - start_step) % devices
    late_owner = (position - start_step - (STEPS - 1)) % devices
    early_loss, early_image, early_sum = pair_tile(
        image_low, early_block, early_owner, match, scale, shift_value
    )
    late_loss, late_image, late_sum = pair_tile(
        image_low, late_block, late_owner, match, scale, shift_value
    )

    def two_turn(turn, carry):
        early_now, late_now, early_acc, late_acc, image_now, loss_now = carry
        early_now = shifted(early_now, ("dp", "tensor"), 1)
        late_now = shifted(late_now, ("dp", "tensor"), -1)
        early_acc = shifted(early_acc, ("dp", "tensor"), 1)
        late_acc = shifted(late_acc, ("dp", "tensor"), -1)
        owner_early = (position - start_step - turn) % devices
        owner_late = (position - start_step - (STEPS - 1) + turn) % devices
        loss_one, image_one, text_one = pair_tile(
            image_low, early_now, owner_early, match, scale, shift_value
        )
        loss_two, image_two, text_two = pair_tile(
            image_low, late_now, owner_late, match, scale, shift_value
        )
        return (
            early_now,
            late_now,
            early_acc + text_one,
            late_acc + text_two,
            image_now + image_one + image_two,
            loss_now + loss_one + loss_two,
        )

    carried = lax.fori_loop(
        1,
        half_steps,
        two_turn,
        (
            early_block,
            late_block,
            early_sum,
            late_sum,
            early_image + late_image,
            early_loss + late_loss,
        ),
    )
    early_sum = carried[2]
    late_sum = carried[3]
    image_dunit = carried[4]
    row_loss = carried[5]
    late_moved = shifted(late_sum, ("dp", "tensor"), -1)
    text_dunit = return_home(early_sum + late_moved, half_steps - 1, window)
    img_grad = (
        image_dunit - img_unit * jnp.sum(img_unit * image_dunit, axis=1, keepdims=True)
    ) / img_len
    txt_grad = (
        text_dunit - txt_unit * jnp.sum(txt_unit * text_dunit, axis=1, keepdims=True)
    ) / txt_len
    return (img_grad, txt_grad, row_loss)


def tangent(dunit, unit, inverse):
    return (dunit - unit * jnp.sum(unit * dunit, axis=1, keepdims=True)) * inverse


def unit_low(emb):
    inverse = 1.0 / jnp.sqrt(jnp.sum(emb * emb, axis=1, keepdims=True) + 1e-06)
    return emb * inverse, inverse


def stable_terms(logit, positive):
    signed = jnp.where(positive, -logit, logit)
    small = jnp.exp(-jnp.abs(signed))
    loss = jnp.maximum(signed, 0.0) + jnp.log1p(small)
    chance = jnp.where(signed >= 0.0, 1.0, small) / (1.0 + small)
    return loss, jnp.where(positive, -chance, chance)


HALVES = 2
TAIL = 32


def plane_kernel(
    log_temp,
    bias,
    window_index,
    match,
    acts,
    txt_proj,
    img_hidden,
    img_down,
    img_pooled,
    img_grad,
    txt_grad,
    row_loss,
    acts_all,
    weights,
    hidden,
    down,
    pooled,
    partial,
    chain_out,
    chain_in,
    img_all,
    img_unit,
    img_inv,
    txt_low,
    txt_unit,
    txt_inv,
    coef_all,
    match_all,
    loss_out,
    loss_in,
    tg_own,
    tg_out,
    tg_in,
    even,
    cross_out,
    cross_in,
    plane_out,
    plane_in,
    loc_sem,
    a_send,
    a_recv,
    w_zsend,
    w_psend,
    w_csend,
    w_recv,
    m_send,
    m_recv,
    c_send,
    c_recv,
    i_send,
    i_fsend,
    i_recv,
    t_send,
    t_recv,
    x_send,
    x_recv,
    p_send,
    p_recv,
    l_send,
    l_recv,
):
    mesh_id = pl.DeviceIdType.MESH
    dp = lax.axis_index("dp")
    z = lax.axis_index("tensor")
    groups = lax.axis_size("dp")
    depth = lax.axis_size("tensor")
    chips = groups // 2
    rows = img_pooled.shape[0]
    width = img_pooled.shape[1]
    piece = rows // HALVES
    chip = dp // 2
    c = dp % 2
    partner = chip * 2 + 1 - c
    y, x = chip // 2, chip % 2
    near = [
        (y * 2 + 1 - x) * 2 + c,
        ((1 - y) * 2 + x) * 2 + c,
        ((1 - y) * 2 + 1 - x) * 2 + c,
    ]
    part_rows = weights.shape[1] // chips
    features = txt_proj.shape[0]
    main = features - TAIL

    local = [
        pltpu.make_async_copy(acts, acts_all.at[z], loc_sem.at[0]),
        pltpu.make_async_copy(txt_proj, weights.at[z, pl.ds(0, features)], loc_sem.at[1]),
        pltpu.make_async_copy(img_hidden, hidden, loc_sem.at[2]),
        pltpu.make_async_copy(img_down, down, loc_sem.at[3]),
        pltpu.make_async_copy(img_pooled, pooled, loc_sem.at[4]),
    ]
    for copy in local:
        copy.start()
    weights[z, pl.ds(features, weights.shape[1] - features)] = jnp.zeros(
        (weights.shape[1] - features, width), weights.dtype
    )

    barrier = pltpu.get_barrier_semaphore()
    for ahead in range(1, groups):
        pl.semaphore_signal(
            barrier, inc=1, device_id=((dp + ahead) % groups, z), device_id_type=mesh_id
        )
    for ahead in range(1, depth):
        pl.semaphore_signal(
            barrier, inc=1, device_id=(dp, (z + ahead) % depth), device_id_type=mesh_id
        )
    pl.semaphore_wait(barrier, groups + depth - 2)

    started = []

    def send(source, target, send_sem, recv_sem, device, when=None):
        def make():
            return pltpu.make_async_remote_copy(
                src_ref=source,
                dst_ref=target,
                send_sem=send_sem,
                recv_sem=recv_sem,
                device_id=device,
                device_id_type=mesh_id,
            )

        if when is None:
            make().start()
        else:

            @pl.when(when)
            def _():
                make().start()

        started.append((when, make))

    def arrive(target, recv_sem):
        pltpu.make_async_remote_copy(
            src_ref=target,
            dst_ref=target,
            send_sem=loc_sem.at[0],
            recv_sem=recv_sem,
            device_id=(partner, z),
            device_id_type=mesh_id,
        ).wait_recv()

    def arrive_when(when, target, recv_sem):
        @pl.when(when)
        def _():
            arrive(target, recv_sem)

    has_up = z < depth - 1
    has_down = z > 0

    local[0].wait()
    send(acts_all.at[z], acts_all.at[z], a_send.at[0, 0], a_recv.at[z], (dp, z + 1), has_up)
    send(acts_all.at[z], acts_all.at[z], a_send.at[1, 0], a_recv.at[z], (dp, z - 1), has_down)
    local[1].wait()
    flow = 1 - 2 * c
    flow_on = jnp.logical_and(z + flow >= 0, z + flow < depth)

    def part(level, index):
        start = pl.multiple_of(index * part_rows, part_rows)
        return weights.at[level, pl.ds(start, part_rows)]

    send(part(z, chip), part(z, chip), w_zsend.at[0], w_recv.at[z, chip], (dp, z + flow), flow_on)
    for ahead in range(1, groups):
        send(
            match,
            match_all.at[dp],
            m_send.at[ahead],
            m_recv.at[dp],
            ((dp + ahead) % groups, z),
        )
    match_all[dp] = match[...]

    upper = z // (depth // 2)
    toward = 1 - 2 * upper
    is_end = jnp.logical_or(z == 0, z == depth - 1)
    is_inner = jnp.logical_not(is_end)

    def mirror(level):
        return level + upper * (depth - 1 - 2 * level)

    local[2].wait()
    local[3].wait()
    local[4].wait()
    for step in range(depth):
        block = mirror(depth - 1 - step)
        partial[block] = jnp.dot(
            hidden[pl.ds(pl.multiple_of(block * rows, rows), rows), :],
            down[...],
            preferred_element_type=jnp.float32,
        )
        if step < depth - 1:

            @pl.when(is_end)
            def _(block=block):
                chain_out[upper, block] = partial[block].astype(chain_out.dtype)

            for h in range(HALVES):
                span = pl.ds(h * piece, piece)
                send(
                    chain_out.at[upper, block, span],
                    chain_in.at[upper, block, span],
                    c_send.at[upper, block, h],
                    c_recv.at[upper, block, h],
                    (dp, z + toward),
                    is_end,
                )

    def spread_weights(hop):
        level = z - flow * hop
        here = jnp.logical_and(level >= 0, level < depth)

        @pl.when(here)
        def _():
            arrive(part(level, chip), w_recv.at[level, chip])

        send(
            part(level, chip),
            part(level, chip),
            w_zsend.at[hop],
            w_recv.at[level, chip],
            (dp, z + flow),
            jnp.logical_and(here, flow_on),
        )
        for job, peer in enumerate(near):
            send(
                part(level, chip),
                part(level, chip),
                w_psend.at[hop, job],
                w_recv.at[level, chip],
                (peer, z),
                here,
            )
        send(
            part(level, chip),
            part(level, chip),
            w_csend.at[hop, 0],
            w_recv.at[level, chip],
            (partner, z),
            here,
        )

    def relay_acts(tag, level, way, forward):
        arrive(acts_all.at[level], a_recv.at[level])
        if forward:
            pltpu.make_async_remote_copy(
                src_ref=acts_all.at[level],
                dst_ref=acts_all.at[level],
                send_sem=a_send.at[way, tag],
                recv_sem=a_recv.at[level],
                device_id=(dp, z + (toward if way == 0 else -toward)),
                device_id_type=mesh_id,
            ).start()

    def relay_sums(block, way):
        lane = upper if way == 0 else 1 - upper
        for h in range(HALVES):
            span = pl.ds(h * piece, piece)
            arrive(chain_in.at[lane, block, span], c_recv.at[lane, block, h])
            chain_out[lane, block, span] = (
                partial[block, span] + chain_in[lane, block, span].astype(jnp.float32)
            ).astype(chain_out.dtype)
            pltpu.make_async_remote_copy(
                src_ref=chain_out.at[lane, block, span],
                dst_ref=chain_in.at[lane, block, span],
                send_sem=c_send.at[lane, block, h],
                recv_sem=c_recv.at[lane, block, h],
                device_id=(dp, z + (toward if way == 0 else -toward)),
                device_id_type=mesh_id,
            ).start()

    def sent(source, send_sem):
        pltpu.make_async_remote_copy(
            src_ref=source,
            dst_ref=source,
            send_sem=send_sem,
            recv_sem=loc_sem.at[0],
            device_id=(partner, z),
            device_id_type=mesh_id,
        ).wait_send()

    m0, m1, m2, m3 = (mirror(level) for level in range(4))
    spread_weights(1)

    @pl.when(is_inner)
    def _():
        relay_acts(1, m0, 0, True)
        relay_acts(1, m2, 1, True)

    spread_weights(2)

    @pl.when(is_inner)
    def _():
        relay_sums(m3, 0)
        relay_acts(2, m3, 1, True)

    spread_weights(3)

    @pl.when(is_inner)
    def _():
        relay_sums(m2, 0)
        relay_sums(m0, 1)

    @pl.when(is_end)
    def _():
        for level in (m1, m2, m3):
            relay_acts(0, level, 0, False)

    for h in range(HALVES):
        span = pl.ds(h * piece, piece)
        from_far = chain_in.at[1 - upper, z, span]
        from_near = chain_in.at[upper, z, span]
        arrive(from_far, c_recv.at[1 - upper, z, h])
        partial[z, span] = partial[z, span] + chain_in[1 - upper, z, span].astype(jnp.float32)

        @pl.when(is_inner)
        def _():
            arrive(from_near, c_recv.at[upper, z, h])
            partial[z, span] = partial[z, span] + chain_in[upper, z, span].astype(jnp.float32)

        unit, inverse = unit_low(partial[z, span] + pooled[span].astype(jnp.float32))
        img_unit[span] = unit
        img_inv[span] = inverse
        img_all[dp, span] = unit.astype(img_all.dtype)
        for job, peer in enumerate(near + [partner]):
            send(
                img_all.at[dp, span],
                img_all.at[dp, span],
                i_send.at[h, job],
                i_recv.at[dp, h],
                (peer, z),
            )

    for hop in range(1, depth):
        level = z - flow * hop
        here = jnp.logical_and(level >= 0, level < depth)
        for job, peer in enumerate(near):
            index = peer // 2
            arrive_when(here, part(level, index), w_recv.at[level, index])
            send(
                part(level, index),
                part(level, index),
                w_csend.at[hop, 1 + job],
                w_recv.at[level, index],
                (partner, z),
                here,
            )
    for hop in range(1, depth):
        level = z + flow * hop
        here = jnp.logical_and(level >= 0, level < depth)
        for index in range(chips):
            arrive_when(here, part(level, index), w_recv.at[level, index])

    lanes = lax.broadcasted_iota(jnp.int32, (rows // 2, main), 1) // TAIL
    repeats = main // TAIL
    for off in range(depth):
        block = (z + off) % depth
        emb = jnp.zeros((rows, width), jnp.float32)
        tails = [jnp.zeros((rows // 2, width), jnp.float32) for _ in range(2)]
        for level in range(depth):
            emb += jnp.dot(
                acts_all[level, pl.ds(pl.multiple_of(block * rows, rows), rows)],
                weights[level, pl.ds(0, main)],
                preferred_element_type=jnp.float32,
            )
            packed = acts_all[level, pl.ds(depth * rows, rows // 2)]
            tail = jnp.concatenate([weights[level, pl.ds(main, TAIL)]] * repeats, axis=0)
            for s in range(2):
                tails[s] += jnp.dot(
                    jnp.where(lanes == 2 * block + s, packed, jnp.zeros_like(packed)),
                    tail,
                    preferred_element_type=jnp.float32,
                )
        unit, inverse = unit_low(emb + jnp.concatenate(tails, axis=0))
        txt_low[pl.ds(off * rows, rows)] = unit.astype(txt_low.dtype)
        if off == 0:
            txt_unit[...] = unit
            txt_inv[...] = inverse

    for h in range(HALVES):
        span = pl.ds(h * piece, piece)
        for job, peer in enumerate(near):
            arrive(img_all.at[peer, span], i_recv.at[peer, h])
            send(
                img_all.at[peer, span],
                img_all.at[peer, span],
                i_fsend.at[h, job],
                i_recv.at[peer, h],
                (partner, z),
            )
    for h in range(HALVES):
        span = pl.ds(h * piece, piece)
        for peer in [partner] + [2 * (p // 2) + 1 - c for p in near]:
            arrive(img_all.at[peer, span], i_recv.at[peer, h])
    for ahead in range(1, groups):
        peer = (dp + ahead) % groups
        arrive(match_all.at[peer], m_recv.at[peer])

    scale = jnp.exp(jnp.full((rows, rows), log_temp[0], jnp.float32))
    shift_value = bias[0]
    window = window_index[0]
    half_groups = groups // 2
    nt = (((1,), (1,)), ((), ()))
    tn = (((0,), (0,)), ((), ()))
    losses = [jnp.zeros((1, rows), jnp.float32) for _ in range(half_groups + 1)]
    for off in (2, 1, 3, 0):
        block = (z + off) % depth
        here = txt_low[pl.ds(off * rows, rows)]
        text_index = (dp * depth + block) * rows + lax.broadcasted_iota(
            jnp.int32, (rows, rows), 0
        )
        beyond = (block > z).astype(jnp.int32)
        far = beyond + window - 2 * beyond * window
        total = jnp.zeros((rows, width), jnp.float32)
        for slot in range(half_groups):
            jump = half_groups * far if slot == 0 else slot + half_groups * window
            who = (dp + jump) % groups
            image = img_all[who]
            cosine = lax.dot_general(here, image, nt, preferred_element_type=jnp.float32)
            logit = scale * cosine + shift_value
            loss, slope = stable_terms(logit, match_all[who] == text_index)
            coef = (slope * scale).astype(jnp.bfloat16)
            total += jnp.dot(coef, image, preferred_element_type=jnp.float32)
            lost = jnp.sum(loss, axis=0, keepdims=True)
            if slot:
                coef_all[slot, pl.ds(off * rows, rows)] = coef
                losses[slot] += lost
            else:
                zero = jnp.zeros_like(coef)
                coef_all[0, pl.ds(off * rows, rows)] = jnp.where(far == 0, coef, zero)
                coef_all[half_groups, pl.ds(off * rows, rows)] = jnp.where(far == 1, coef, zero)
                losses[0] += jnp.where(far == 0, lost, 0.0)
                losses[half_groups] += jnp.where(far == 1, lost, 0.0)
        if off:
            tg_out[off] = total.astype(tg_out.dtype)
            send(tg_out.at[off], tg_in.at[off], t_send.at[off], t_recv.at[off], (dp, block))
        else:
            tg_own[...] = total

    first = window == 0
    for jump in range(groups):
        if jump % half_groups == 0:
            value = losses[jump]
        else:
            value = jnp.where(first if jump < half_groups else window == 1, losses[jump % half_groups], 0.0)
        loss_out[jump] = value
    for jump in range(1, groups):
        send(
            loss_out.at[jump],
            loss_in.at[jump],
            l_send.at[jump],
            l_recv.at[jump],
            ((dp + jump) % groups, z),
        )

    def image_sum(slot):
        return lax.dot_general(
            coef_all[slot], txt_low[...], tn, preferred_element_type=jnp.float32
        )

    for slot in (1, 3):
        value = image_sum(slot)
        for late in (0, 1):
            lane = ((slot - 1) // 2 + 2 * late + c) % chips
            kept = jnp.where(window == late, value, 0.0)
            cross_out[lane] = kept.astype(cross_out.dtype)
            send(
                cross_out.at[lane],
                cross_in.at[lane],
                x_send.at[lane],
                x_recv.at[lane],
                (partner, z),
            )
    value = image_sum(2)
    even[1] = jnp.where(window == 0, value, 0.0)
    even[3] = jnp.where(window == 1, value, 0.0)
    even[2] = image_sum(half_groups)
    even[0] = image_sum(0)
    for lane in (1, 2, 3):
        arrive(cross_in.at[lane], x_recv.at[lane])
        plane_out[lane] = (even[lane] + cross_in[lane].astype(jnp.float32)).astype(plane_out.dtype)
        send(
            plane_out.at[lane],
            plane_in.at[lane],
            p_send.at[lane],
            p_recv.at[lane],
            (((chip + lane) % chips) * 2 + c, z),
        )
    arrive(cross_in.at[0], x_recv.at[0])
    dunit = even[0] + cross_in[0].astype(jnp.float32)
    total = loss_out[0]
    for jump in range(1, groups):
        arrive(loss_in.at[jump], l_recv.at[jump])
        total += loss_in[jump]
    row_loss[...] = total
    for lane in (1, 2, 3):
        arrive(plane_in.at[lane], p_recv.at[lane])
        dunit += plane_in[lane].astype(jnp.float32)
    img_grad[...] = tangent(dunit, img_unit[...], img_inv[...])
    dunit = tg_own[...]
    for off in (1, 2, 3):
        arrive(tg_in.at[off], t_recv.at[off])
        dunit += tg_in[off].astype(jnp.float32)
    txt_grad[...] = tangent(dunit, txt_unit[...], txt_inv[...])

    for when, make in started:
        if when is None:
            make().wait_send()
        else:

            @pl.when(when)
            def _():
                make().wait_send()

    @pl.when(is_inner)
    def _():
        sent(acts_all.at[m0], a_send.at[0, 1])
        sent(acts_all.at[m2], a_send.at[1, 1])
        sent(acts_all.at[m3], a_send.at[1, 2])
        for block, way in ((m3, 0), (m2, 0), (m0, 1)):
            lane = upper if way == 0 else 1 - upper
            for h in range(HALVES):
                span = pl.ds(h * piece, piece)
                sent(chain_out.at[lane, block, span], c_send.at[lane, block, h])


def plane_body(
    img_hidden, img_down, img_pooled, txt_hidden, txt_proj, log_temp, bias, match, window_index
):
    groups = lax.axis_size("dp")
    depth = lax.axis_size("tensor")
    chips = groups // 2
    rows, width = img_pooled.shape
    features = txt_hidden.shape[1]
    main = features - TAIL
    fold = main // TAIL
    packed = (
        txt_hidden[:, main:]
        .reshape(fold, depth * rows // fold, TAIL)
        .transpose(1, 0, 2)
        .reshape(depth * rows // fold, main)
    )
    acts = jnp.concatenate([txt_hidden[:, :main], packed], axis=0)
    padded = -(-features // (16 * chips)) * 16 * chips
    dma = pltpu.SemaphoreType.DMA
    low, full = jnp.bfloat16, jnp.float32
    vmem = pltpu.VMEM
    smem = pl.BlockSpec(memory_space=pltpu.SMEM)
    inside = pl.BlockSpec(memory_space=pltpu.VMEM)
    anywhere = pl.BlockSpec(memory_space=pl.ANY)
    block = (rows, width)
    img_grad, txt_grad, row_loss = pl.pallas_call(
        plane_kernel,
        out_shape=(
            jax.ShapeDtypeStruct(block, full),
            jax.ShapeDtypeStruct(block, full),
            jax.ShapeDtypeStruct((1, rows), full),
        ),
        in_specs=[smem, smem, smem, inside] + [anywhere] * 5,
        out_specs=(inside, inside, inside),
        scratch_shapes=[
            vmem((depth,) + acts.shape, low),
            vmem((depth, padded, width), low),
            vmem(img_hidden.shape, low),
            vmem(img_down.shape, low),
            vmem(block, low),
            vmem((depth,) + block, full),
            vmem((2, depth) + block, low),
            vmem((2, depth) + block, low),
            vmem((groups,) + block, low),
            vmem(block, full),
            vmem((rows, 1), full),
            vmem((depth * rows, width), low),
            vmem(block, full),
            vmem((rows, 1), full),
            vmem((groups // 2 + 1, depth * rows, rows), low),
            vmem((groups, 1, rows), jnp.int32),
            vmem((groups, 1, rows), full),
            vmem((groups, 1, rows), full),
            vmem(block, full),
            vmem((depth,) + block, low),
            vmem((depth,) + block, low),
            vmem((chips,) + block, full),
            vmem((chips,) + block, low),
            vmem((chips,) + block, low),
            vmem((chips,) + block, low),
            vmem((chips,) + block, low),
            dma((5,)),
            dma((2, depth)),
            dma((depth,)),
            dma((depth,)),
            dma((depth, 3)),
            dma((depth, 4)),
            dma((depth, chips)),
            dma((groups,)),
            dma((groups,)),
            dma((2, depth, HALVES)),
            dma((2, depth, HALVES)),
            dma((HALVES, 4)),
            dma((HALVES, 3)),
            dma((groups, HALVES)),
            dma((depth,)),
            dma((depth,)),
            dma((chips,)),
            dma((chips,)),
            dma((chips,)),
            dma((chips,)),
            dma((groups,)),
            dma((groups,)),
        ],
        compiler_params=pltpu.CompilerParams(
            collective_id=1, has_side_effects=True, vmem_limit_bytes=60 * 1024 * 1024
        ),
        name="plane",
    )(
        log_temp,
        bias,
        window_index,
        match.reshape(1, rows),
        acts,
        txt_proj,
        img_hidden,
        img_down,
        img_pooled,
    )
    return img_grad, txt_grad, row_loss.reshape(rows)


def solution(mesh):
    in_specs = (
        P("dp", "tensor"),
        P("tensor", None),
        P(("dp", "tensor"), None),
        P("dp", "tensor"),
        P("tensor", None),
        P(),
        P(),
        P(("dp", "tensor")),
        P(),
    )
    out_specs = (P(("dp", "tensor"), None), P(("dp", "tensor"), None), P(("dp", "tensor")))
    whole = mesh.shape["dp"] * mesh.shape["tensor"]
    body = plane_body if whole == 2 * STEPS and mesh.shape["dp"] == 8 and mesh.shape["tensor"] == 4 else ring_body
    return jax.shard_map(body, mesh=mesh, in_specs=in_specs, out_specs=out_specs, check_vma=False)
```
